128 devices in a mesh: lat: 2 (over core), lon: 8 (over y, x_hi), lev: 8 (over z, x_lo).
Axes of the slice: x: 4 (x_hi: 2, x_lo: 2; x = x_hi * 2 + x_lo), y: 4, z: 4, core: 2. Of those that a mesh axis runs over, the one named last changes fastest.
Arguments:
- field_values: float32 [16, 1024, 128, 128], P('lat', 'lon', 'lev'), may hold values from 0.2 to 1.8
- crowding: float32 [16, 1024, 128, 128], P('lat', 'lon', 'lev'), may hold values from 0.5 to 2
Outputs:
- potential: float32 [16, 1024, 128, 128], P('lat', 'lon', 'lev')
- field_values_end: float32 [16, 1024, 128, 128], P('lat', 'lon', 'lev')
The draws below stay inside these ranges and needn't reach their ends.
All inputs are finite; a program needn't handle non-finite values.
Results may differ from the reference program's by a relative error of at most 0.00002.
Values sent between devices are 32-bit elements; how exact they have to be, the bound alone decides.
A program may use at most 256 MiB of HBM per device.

```python
import jax
import jax.numpy as jnp
from jax import lax

GRID_Y = 16
GRID_X = 1024
GRID_Z = 128
LEVELS = 128
STEPS = 4


def block_levels(rng, shape, split, low, top_value):
    def one(axis_at, parts):
        heights = jax.random.uniform(jax.random.fold_in(jax.random.fold_in(rng, 6), axis_at), (parts,), jnp.float32, low / len(split), top_value / len(split))
        return jnp.repeat(jnp.exp(heights), shape[axis_at] // parts).reshape((-1,) + (1,) * (len(shape) - axis_at - 1))

    gain = one(*split[0])
    for cut in split[1:]:
        gain = gain * one(*cut)
    return gain


def setup_inputs(seed: int = 0) -> dict:
    splits = jax.random.split(jax.random.key(seed), 3)
    field_values = jnp.clip(0.2 + 1.5999999 * jax.random.uniform(splits[0], (GRID_Y, GRID_X, GRID_Z, LEVELS), jnp.float32) ** block_levels(splits[0], (GRID_Y, GRID_X, GRID_Z, LEVELS), ((0, 2), (1, 8), (2, 8)), -0.2, 0.2), 0.2, 1.8)
    crowding = jnp.clip(0.5 + 1.5 * jax.random.uniform(splits[1], (GRID_Y, GRID_X, GRID_Z, LEVELS), jnp.float32) ** block_levels(splits[1], (GRID_Y, GRID_X, GRID_Z, LEVELS), ((0, 2), (1, 8), (2, 8)), -0.2, 0.2), 0.5, 2.0)
    return {"field_values": field_values, "crowding": crowding}


def without_rim(values, dims):
    for dim in dims:
        values = lax.slice_in_dim(values, 1, values.shape[dim] - 1, axis=dim)
    return values


def shifted_cells(values, dim, start, dims):
    others = [other for other in dims if other != dim]
    values = without_rim(values, others)
    return lax.slice_in_dim(values, start, start + values.shape[dim] - 2, axis=dim)


def march_step(padded, crowding):
    middle = without_rim(padded, (0, 1, 2))
    lower = [shifted_cells(padded, dim, 0, (0, 1, 2)) for dim in (0, 1, 2)]
    upper = [shifted_cells(padded, dim, 2, (0, 1, 2)) for dim in (0, 1, 2)]
    spread = lower[0] + upper[0] + lower[1] + upper[1] + lower[2] + upper[2] - 6.0 * middle
    return middle + 0.1 * spread + 0.2 * middle * (1.0 - middle * crowding)


def reference(field_values, crowding):
    for step in range(STEPS):
        field_values = march_step(jnp.pad(field_values, ((1, 1), (1, 1), (1, 1), (0, 0)), mode="wrap"), crowding)
    potential = jnp.cumsum(field_values, axis=2) / GRID_Z
    return potential, field_values
```

```python
import functools

import jax
import jax.numpy as jnp
from jax import lax
from jax.experimental import pallas as pl
from jax.experimental.pallas import tpu as pltpu
from jax.sharding import PartitionSpec as P

STEPS = 4
GROUP = 8
MESH = pl.DeviceIdType.MESH


def kernel(
    width, scale, field_hbm, crowd_hbm, pot, end,
    F, C, H, S, T, Q, R, X, B,
    ld_f, ld_c, z_send, z_recv, y_send, y_recv, x_send, x_recv, q_send, q_recv, b_send, b_recv,
):
    ny, nx, nz, _ = field_hbm.shape
    chunks = nx // width
    lat, lon, lev = (lax.axis_index(a) for a in ("lat", "lon", "lev"))
    n_lon, n_lev = lax.axis_size("lon"), lax.axis_size("lev")
    levels = n_lev // 2
    at_z, at_x = lax.div(lev, 2), lax.rem(lev, 2)
    up = (lat, lon, lax.rem(lev + 1, n_lev))
    down = (lat, lon, lax.rem(lev + n_lev - 1, n_lev))
    right = (lat, lax.rem(lon + 1, n_lon), lev)
    left = (lat, lax.rem(lon + n_lon - 1, n_lon), lev)
    core = (1 - lat, lon, lev)
    above = (lat, lon, lax.rem(lev + 2, n_lev))
    beneath = (lat, lon, lax.rem(lev + n_lev - 2, n_lev))
    partner = (lat, lon, lev + 1 - 2 * at_x)

    def load_field(c):
        columns = pl.ds(c * width, width)
        inside = pl.ds(c * width + 1, width)
        return pltpu.make_async_copy(
            field_hbm.at[:, columns], F.at[0, pl.ds(1, ny), inside], ld_f.at[c]
        )

    def load_crowding(c):
        columns = pl.ds(c * width, width)
        return pltpu.make_async_copy(crowd_hbm.at[:, columns], C.at[:, columns], ld_c.at[c])

    def in_turn(i):
        return lax.rem(i + (chunks - 1), chunks)

    def start_loads(i, carry):
        load_field(in_turn(i)).start()
        return carry

    lax.fori_loop(0, chunks, start_loads, 0)

    def start_crowding(i, carry):
        load_crowding(in_turn(i)).start()
        return carry

    lax.fori_loop(0, chunks, start_crowding, 0)

    @pl.when(at_z == 0)
    def _():
        def clear(c, carry):
            Q[c] = jnp.zeros(Q.shape[1:], Q.dtype)
            return carry

        lax.fori_loop(0, chunks, clear, 0)

    barrier = pltpu.get_barrier_semaphore()
    peers = (up, down, right, left, core, above, beneath)
    for peer in peers:
        pl.semaphore_signal(barrier, inc=1, device_id=peer, device_id_type=MESH)
    pl.semaphore_wait(barrier, len(peers))

    def remote(src, dst, send, recv, to):
        return pltpu.make_async_remote_copy(
            src_ref=src, dst_ref=dst, send_sem=send, recv_sem=recv, device_id=to, device_id_type=MESH
        )

    def faces(p, c):
        inside = pl.ds(c * width + 1, width)
        return (
            remote(S.at[p, 1, c], H.at[p, 0, c], z_send.at[p, 0, c], z_recv.at[p, 0, c], up),
            remote(S.at[p, 0, c], H.at[p, 1, c], z_send.at[p, 1, c], z_recv.at[p, 1, c], down),
            remote(F.at[p, ny, inside], F.at[p, 0, inside], y_send.at[p, 0, c], y_recv.at[p, 0, c], core),
            remote(F.at[p, 1, inside], F.at[p, ny + 1, inside], y_send.at[p, 1, c], y_recv.at[p, 1, c], core),
        )

    def right_face(p):
        rows = pl.ds(1, ny)
        return remote(F.at[p, rows, nx], F.at[p, rows, 0], x_send.at[p, 0], x_recv.at[p, 0], right)

    def left_face(p):
        rows = pl.ds(1, ny)
        return remote(F.at[p, rows, 1], F.at[p, rows, nx + 1], x_send.at[p, 1], x_recv.at[p, 1], left)

    def start_faces(p, c):
        @pl.when(c == chunks - 1)
        def _():
            right_face(p).start()

        @pl.when(c == 0)
        def _():
            left_face(p).start()

        for copy in faces(p, c):
            copy.start()

    def await_faces(p, c):
        for copy in faces(p, c):
            copy.wait_recv()

        @pl.when(c == 0)
        def _():
            right_face(p).wait_recv()

        @pl.when(c == chunks - 1)
        def _():
            left_face(p).wait_recv()

    def await_sent(p, c):
        for copy in faces(p, c):
            copy.wait_send()

        @pl.when(c == chunks - 1)
        def _():
            right_face(p).wait_send()

        @pl.when(c == 0)
        def _():
            left_face(p).wait_send()

    groups = width // GROUP

    def over_groups(c, body):
        def row(y, carry):
            def group(g, inner):
                body(y, g * GROUP, c * width + g * GROUP)
                return inner

            return lax.fori_loop(0, groups, group, carry)

        lax.fori_loop(0, ny, row, 0)

    def compute(step, c):
        p = step % 2
        level = lax.broadcasted_iota(jnp.int32, (nz, 128), 0)

        def body(y, g, x):
            columns = [F[p, y + 1, x + j] for j in range(GROUP + 2)]
            for j in range(GROUP):
                middle = columns[j + 1]
                low = H[p, 0, c, y, pl.ds(g + j, 1), :]
                high = H[p, 1, c, y, pl.ds(g + j, 1), :]
                under = jnp.where(level == 0, low, pltpu.roll(middle, 1, 0))
                over = jnp.where(level == nz - 1, high, pltpu.roll(middle, nz - 1, 0))
                total = columns[j] + columns[j + 2] + F[p, y, x + j + 1] + F[p, y + 2, x + j + 1] + under + over
                new = 0.1 * total + middle * (0.6 - 0.2 * (middle * C[y, x + j]))
                if step < STEPS - 1:
                    F[1 - p, y + 1, x + j + 1] = new
                    S[1 - p, 0, c, y, pl.ds(g + j, 1), :] = new[0:1]
                    S[1 - p, 1, c, y, pl.ds(g + j, 1), :] = new[nz - 1 : nz]
                else:
                    end[y, x + j] = new
                    here = new
                    reach = 1
                    while reach < nz:
                        here = here + jnp.where(level >= reach, pltpu.roll(here, reach, 0), 0.0)
                        reach *= 2
                    pot[y, x + j] = here * scale
                    T[c, y, pl.ds(g + j, 1), :] = here[nz - 1 : nz]

        over_groups(c, body)

    def first(i, carry):
        c = in_turn(i)
        load_field(c).wait()

        def body(y, g, x):
            for j in range(GROUP):
                value = F[0, y + 1, x + j + 1]
                S[0, 0, c, y, pl.ds(g + j, 1), :] = value[0:1]
                S[0, 1, c, y, pl.ds(g + j, 1), :] = value[nz - 1 : nz]

        over_groups(c, body)
        start_faces(0, c)
        return carry

    lax.fori_loop(0, chunks, first, 0)

    def upward(c):
        return remote(R.at[c], Q.at[c], q_send.at[c], q_recv.at[c], above)

    def across(c):
        return remote(X.at[c], B.at[c], b_send.at[c], b_recv.at[c], partner)

    def chain(c):
        @pl.when(at_z > 0)
        def _():
            upward(c).wait_recv()

        before = Q[c]
        through = before + T[c]
        R[c] = through
        X[c] = jnp.where(at_x == 0, through, before)

        @pl.when(at_z < levels - 1)
        def _():
            upward(c).start()

        across(c).start()

    for step in range(STEPS):
        p = step % 2

        def advance(i, carry):
            c = in_turn(i)
            if step == 0:
                load_crowding(c).wait()
            else:
                await_sent(1 - p, c)
            await_faces(p, c)
            compute(step, c)
            if step < STEPS - 1:
                start_faces(1 - p, c)
            else:
                chain(c)
            return carry

        lax.fori_loop(0, chunks, advance, 0)

    def finish(i, carry):
        c = in_turn(i)
        across(c).wait_recv()
        T[c] = (Q[c] + B[c]) * scale

        def body(y, g, x):
            for j in range(GROUP):
                pot[y, x + j] = pot[y, x + j] + T[c, y, pl.ds(g + j, 1), :]

        over_groups(c, body)
        return carry

    lax.fori_loop(0, chunks, finish, 0)

    def drain(i, carry):
        c = in_turn(i)
        await_sent((STEPS - 1) % 2, c)
        across(c).wait_send()

        @pl.when(at_z < levels - 1)
        def _():
            upward(c).wait_send()

        return carry

    lax.fori_loop(0, chunks, drain, 0)


def per_device(field_values, crowding):
    ny, nx, nz, lanes = field_values.shape
    width = min(16, nx // 2)
    chunks = nx // width
    scale = 1.0 / (nz * lax.axis_size("lev"))
    f32 = jnp.float32
    plane = (chunks, ny, width, lanes)
    dma = pltpu.SemaphoreType.DMA
    hbm = pl.BlockSpec(memory_space=pltpu.HBM)
    vmem = pl.BlockSpec(memory_space=pltpu.VMEM)
    return pl.pallas_call(
        functools.partial(kernel, width, scale),
        out_shape=(pltpu.VMEM(field_values.shape, f32), pltpu.VMEM(field_values.shape, f32)),
        in_specs=[hbm, hbm],
        out_specs=(vmem, vmem),
        scratch_shapes=[
            pltpu.VMEM((2, ny + 2, nx + 2, nz, lanes), f32),
            pltpu.VMEM(field_values.shape, f32),
            pltpu.VMEM((2, 2) + plane, f32),
            pltpu.VMEM((2, 2) + plane, f32),
            pltpu.VMEM(plane, f32),
            pltpu.VMEM(plane, f32),
            pltpu.VMEM(plane, f32),
            pltpu.VMEM(plane, f32),
            pltpu.VMEM(plane, f32),
            dma((chunks,)), dma((chunks,)),
            dma((2, 2, chunks)), dma((2, 2, chunks)),
            dma((2, 2, chunks)), dma((2, 2, chunks)),
            dma((2, 2)), dma((2, 2)),
            dma((chunks,)), dma((chunks,)),
            dma((chunks,)), dma((chunks,)),
        ],
        compiler_params=pltpu.CompilerParams(
            collective_id=0, has_side_effects=True, vmem_limit_bytes=42 * 2**20
        ),
    )(field_values, crowding)


def solution(mesh):
    spec = P("lat", "lon", "lev", None)
    return jax.shard_map(
        per_device, mesh=mesh, in_specs=(spec, spec), out_specs=(spec, spec), check_vma=False
    )
```

```python
import functools

import jax
import jax.numpy as jnp
from jax import lax
from jax.experimental import pallas as pl
from jax.experimental.pallas import tpu as pltpu
from jax.sharding import PartitionSpec as P

STEPS = 4
GROUP = 8
MESH = pl.DeviceIdType.MESH


def kernel(
    width, scale, field_hbm, crowd_hbm, pot, end,
    F, C, H, S, T, Q, R, U, V, X, B,
    met, ld_f, ld_c, z_send, z_recv, y_send, y_recv, x_send, x_recv, q_send, q_recv, b_send, b_recv,
):
    ny, nx, nz, _ = field_hbm.shape
    chunks = nx // width
    ahead = chunks // 2
    lat, lon, lev = (lax.axis_index(a) for a in ("lat", "lon", "lev"))
    n_lon, n_lev = lax.axis_size("lon"), lax.axis_size("lev")
    assert n_lev == 8
    at_z, at_x = lax.div(lev, 2), lax.rem(lev, 2)
    up = (lat, lon, lax.rem(lev + 1, n_lev))
    down = (lat, lon, lax.rem(lev + n_lev - 1, n_lev))
    right = (lat, lax.rem(lon + 1, n_lon), lev)
    left = (lat, lax.rem(lon + n_lon - 1, n_lon), lev)
    core = (1 - lat, lon, lev)
    above = (lat, lon, lax.rem(lev + 2, n_lev))
    beneath = (lat, lon, lax.rem(lev + n_lev - 2, n_lev))
    partner = (lat, lon, lev + 1 - 2 * at_x)

    barrier = pltpu.get_barrier_semaphore()
    early = (down, left, core)
    for peer in early:
        pl.semaphore_signal(barrier, inc=1, device_id=peer, device_id_type=MESH)

    def load_field(c):
        columns = pl.ds(c * width, width)
        inside = pl.ds(c * width + 1, width)
        return pltpu.make_async_copy(
            field_hbm.at[:, columns], F.at[0, pl.ds(1, ny), inside], ld_f.at[c]
        )

    def load_crowding(c):
        columns = pl.ds(c * width, width)
        return pltpu.make_async_copy(crowd_hbm.at[:, columns], C.at[:, columns], ld_c.at[c])

    def in_turn(i):
        return lax.rem(i + (chunks - 1), chunks)

    def start_loads(i, carry):
        load_field(in_turn(i)).start()
        return carry

    lax.fori_loop(0, chunks, start_loads, 0)

    def start_crowding(i, carry):
        load_crowding(in_turn(i)).start()
        return carry

    lax.fori_loop(0, chunks, start_crowding, 0)

    def remote(src, dst, send, recv, to):
        return pltpu.make_async_remote_copy(
            src_ref=src, dst_ref=dst, send_sem=send, recv_sem=recv, device_id=to, device_id_type=MESH
        )

    def faces(p, c):
        inside = pl.ds(c * width + 1, width)
        return (
            remote(S.at[p, 1, c], H.at[p, 0, c], z_send.at[p, 0, c], z_recv.at[p, 0, c], up),
            remote(S.at[p, 0, c], H.at[p, 1, c], z_send.at[p, 1, c], z_recv.at[p, 1, c], down),
            remote(F.at[p, ny, inside], F.at[p, 0, inside], y_send.at[p, 0, c], y_recv.at[p, 0, c], core),
            remote(F.at[p, 1, inside], F.at[p, ny + 1, inside], y_send.at[p, 1, c], y_recv.at[p, 1, c], core),
        )

    def right_face(p):
        rows = pl.ds(1, ny)
        return remote(F.at[p, rows, nx], F.at[p, rows, 0], x_send.at[p, 0], x_recv.at[p, 0], right)

    def left_face(p):
        rows = pl.ds(1, ny)
        return remote(F.at[p, rows, 1], F.at[p, rows, nx + 1], x_send.at[p, 1], x_recv.at[p, 1], left)

    def start_onward(p, c):
        @pl.when(c == chunks - 1)
        def _():
            right_face(p).start()

        for k in (0, 2, 3):
            faces(p, c)[k].start()

    def start_back(p, c):
        @pl.when(c == 0)
        def _():
            left_face(p).start()

        faces(p, c)[1].start()

    def start_faces(p, c):
        @pl.when(c == chunks - 1)
        def _():
            right_face(p).start()

        @pl.when(c == 0)
        def _():
            left_face(p).start()

        for copy in faces(p, c):
            copy.start()

    def await_faces(p, c):
        for copy in faces(p, c):
            copy.wait_recv()

        @pl.when(c == 0)
        def _():
            right_face(p).wait_recv()

        @pl.when(c == chunks - 1)
        def _():
            left_face(p).wait_recv()

    def await_sent(p, c):
        for copy in faces(p, c):
            copy.wait_send()

        @pl.when(c == chunks - 1)
        def _():
            right_face(p).wait_send()

        @pl.when(c == 0)
        def _():
            left_face(p).wait_send()

    groups = width // GROUP

    def over_groups(c, body):
        def row(y, carry):
            def group(g, inner):
                body(y, g * GROUP, c * width + g * GROUP)
                return inner

            return lax.fori_loop(0, groups, group, carry)

        lax.fori_loop(0, ny, row, 0)

    def compute(step, c):
        p = step % 2
        level = lax.broadcasted_iota(jnp.int32, (nz, 128), 0)

        def body(y, g, x):
            columns = [F[p, y + 1, x + j] for j in range(GROUP + 2)]
            for j in range(GROUP):
                middle = columns[j + 1]
                low = H[p, 0, c, y, pl.ds(g + j, 1), :]
                high = H[p, 1, c, y, pl.ds(g + j, 1), :]
                under = jnp.where(level == 0, low, pltpu.roll(middle, 1, 0))
                over = jnp.where(level == nz - 1, high, pltpu.roll(middle, nz - 1, 0))
                total = columns[j] + columns[j + 2] + F[p, y, x + j + 1] + F[p, y + 2, x + j + 1] + under + over
                new = 0.1 * total + middle * (0.6 - 0.2 * (middle * C[y, x + j]))
                if step < STEPS - 1:
                    F[1 - p, y + 1, x + j + 1] = new
                    S[1 - p, 0, c, y, pl.ds(g + j, 1), :] = new[0:1]
                    S[1 - p, 1, c, y, pl.ds(g + j, 1), :] = new[nz - 1 : nz]
                else:
                    end[y, x + j] = new
                    here = new
                    reach = 1
                    while reach < nz:
                        here = here + jnp.where(level >= reach, pltpu.roll(here, reach, 0), 0.0)
                        reach *= 2
                    pot[y, x + j] = here * scale
                    T[c, y, pl.ds(g + j, 1), :] = here[nz - 1 : nz]

        over_groups(c, body)

    def prepare(c):
        load_field(c).wait()

        def body(y, g, x):
            for j in range(GROUP):
                value = F[0, y + 1, x + j + 1]
                S[0, 0, c, y, pl.ds(g + j, 1), :] = value[0:1]
                S[0, 1, c, y, pl.ds(g + j, 1), :] = value[nz - 1 : nz]

        over_groups(c, body)

    prepare(in_turn(0))
    pl.semaphore_wait(barrier, len(early))
    pl.semaphore_signal(met.at[0], inc=1, device_id=up, device_id_type=MESH)
    pl.semaphore_signal(met.at[1], inc=1, device_id=right, device_id_type=MESH)
    start_onward(0, in_turn(0))

    def first_onward(i, carry):
        c = in_turn(i)
        prepare(c)
        start_onward(0, c)
        return carry

    def first_back(i, carry):
        start_back(0, in_turn(i))
        return carry

    def first_both(i, carry):
        c = in_turn(i)
        prepare(c)
        start_faces(0, c)
        return carry

    lax.fori_loop(1, ahead, first_onward, 0)
    pl.semaphore_wait(met.at[0], 1)
    pl.semaphore_wait(met.at[1], 1)
    lax.fori_loop(0, ahead, first_back, 0)
    lax.fori_loop(ahead, chunks, first_both, 0)

    def sent_on(src, dst, k, c, to):
        return remote(src.at[c], dst.at[c], q_send.at[k, c], q_recv.at[k, c], to)

    def across(c):
        return remote(X.at[c], B.at[c], b_send.at[c], b_recv.at[c], partner)

    def chain_own(c):
        @pl.when(at_z < 2)
        def _():
            sent_on(T, Q, 0, c, above).start()

        @pl.when(at_z == 0)
        def _():
            sent_on(T, Q, 1, c, beneath).start()

    def chain_first(c):
        @pl.when(at_z == 1)
        def _():
            sent_on(T, Q, 0, c, above).wait_recv()

        @pl.when(at_z == 2)
        def _():
            sent_on(T, Q, 0, c, above).wait_recv()
            U[c] = Q[c] + T[c]
            sent_on(U, R, 0, c, above).start()

        @pl.when(at_z == 3)
        def _():
            sent_on(T, Q, 1, c, beneath).wait_recv()
            sent_on(Q, R, 1, c, beneath).start()

    def chain_second(c):
        @pl.when(at_z == 0)
        def _():
            V[c] = jnp.zeros(V.shape[1:], V.dtype)

        @pl.when(at_z == 1)
        def _():
            V[c] = Q[c]

        @pl.when(at_z == 2)
        def _():
            sent_on(Q, R, 1, c, beneath).wait_recv()
            V[c] = Q[c] + R[c]

        @pl.when(at_z == 3)
        def _():
            sent_on(U, R, 0, c, above).wait_recv()
            V[c] = Q[c] + R[c]

        before = V[c]
        X[c] = jnp.where(at_x == 0, before + T[c], before)
        across(c).start()

    for step in range(STEPS):
        p = step % 2

        def advance(i, carry):
            c = in_turn(i)
            if step == 0:
                load_crowding(c).wait()
            else:
                await_sent(1 - p, c)
            await_faces(p, c)
            compute(step, c)
            if step < STEPS - 1:
                start_faces(1 - p, c)
            else:
                chain_own(c)

                @pl.when(i >= 1)
                def _():
                    chain_first(in_turn(i - 1))

                @pl.when(i >= 2)
                def _():
                    chain_second(in_turn(i - 2))

            return carry

        lax.fori_loop(0, chunks, advance, 0)

    chain_first(in_turn(chunks - 1))
    chain_second(in_turn(chunks - 2))
    chain_second(in_turn(chunks - 1))

    def finish(i, carry):
        c = in_turn(i)
        across(c).wait_recv()
        V[c] = (V[c] + B[c]) * scale

        def body(y, g, x):
            for j in range(GROUP):
                pot[y, x + j] = pot[y, x + j] + V[c, y, pl.ds(g + j, 1), :]

        over_groups(c, body)
        return carry

    lax.fori_loop(0, chunks, finish, 0)

    def drain(i, carry):
        c = in_turn(i)
        await_sent((STEPS - 1) % 2, c)
        across(c).wait_send()

        @pl.when(at_z != 3)
        def _():
            sent_on(T, Q, 0, c, above).wait_send()

        @pl.when((at_z == 0) | (at_z == 3))
        def _():
            sent_on(T, Q, 1, c, beneath).wait_send()

        return carry

    lax.fori_loop(0, chunks, drain, 0)


def put_out(pot, end, pot_out, end_out, sems):
    pieces = sems.shape[1]
    depth = pot.shape[0] // pieces
    copies = [
        pltpu.make_async_copy(src.at[pl.ds(k * depth, depth)], dst.at[pl.ds(k * depth, depth)], sems.at[i, k])
        for k in range(pieces)
        for i, (src, dst) in enumerate(((pot, pot_out), (end, end_out)))
    ]
    for copy in copies:
        copy.start()
    for copy in copies:
        copy.wait()


def per_device(field_values, crowding):
    ny, nx, nz, lanes = field_values.shape
    width = min(16, nx // 2)
    chunks = nx // width
    scale = 1.0 / (nz * lax.axis_size("lev"))
    f32 = jnp.float32
    plane = (chunks, ny, width, lanes)
    dma = pltpu.SemaphoreType.DMA
    hbm = pl.BlockSpec(memory_space=pltpu.HBM)
    vmem = pl.BlockSpec(memory_space=pltpu.VMEM)
    results = pl.pallas_call(
        functools.partial(kernel, width, scale),
        out_shape=(pltpu.VMEM(field_values.shape, f32), pltpu.VMEM(field_values.shape, f32)),
        in_specs=[hbm, hbm],
        out_specs=(vmem, vmem),
        scratch_shapes=[
            pltpu.VMEM((2, ny + 2, nx + 2, nz, lanes), f32),
            pltpu.VMEM(field_values.shape, f32),
            pltpu.VMEM((2, 2) + plane, f32),
            pltpu.VMEM((2, 2) + plane, f32),
            pltpu.VMEM(plane, f32),
            pltpu.VMEM(plane, f32),
            pltpu.VMEM(plane, f32),
            pltpu.VMEM(plane, f32),
            pltpu.VMEM(plane, f32),
            pltpu.VMEM(plane, f32),
            pltpu.VMEM(plane, f32),
            pltpu.SemaphoreType.REGULAR((2,)),
            dma((chunks,)), dma((chunks,)),
            dma((2, 2, chunks)), dma((2, 2, chunks)),
            dma((2, 2, chunks)), dma((2, 2, chunks)),
            dma((2, 2)), dma((2, 2)),
            dma((2, chunks)), dma((2, chunks)),
            dma((chunks,)), dma((chunks,)),
        ],
        compiler_params=pltpu.CompilerParams(
            collective_id=0, has_side_effects=True, vmem_limit_bytes=42 * 2**20
        ),
    )(field_values, crowding)
    shape = jax.ShapeDtypeStruct(field_values.shape, f32)
    pieces = 4
    return tuple(pl.pallas_call(
        put_out,
        out_shape=(shape, shape),
        in_specs=[vmem, vmem],
        out_specs=(hbm, hbm),
        scratch_shapes=[dma((2, pieces))],
        compiler_params=pltpu.CompilerParams(vmem_limit_bytes=2**20),
    )(*results))


def solution(mesh):
    spec = P("lat", "lon", "lev", None)
    return jax.shard_map(
        per_device, mesh=mesh, in_specs=(spec, spec), out_specs=(spec, spec), check_vma=False
    )
```

```python
import functools

import jax
import jax.numpy as jnp
from jax import lax
from jax.experimental import pallas as pl
from jax.experimental.pallas import tpu as pltpu
from jax.sharding import PartitionSpec as P

STEPS = 4
GROUP = 8
LAG = 4
MESH = pl.DeviceIdType.MESH


def kernel(
    width, scale, field_hbm, crowd_hbm, pot, end,
    F, C, H, S, T, Q, R, U, V, X, B,
    met, ld, f_send, f_recv, x_recv, q_send, q_recv, b_send, b_recv,
):
    ny, nx, nz, _ = field_hbm.shape
    chunks = nx // width
    ahead = chunks // 2
    lag = LAG
    lat, lon, lev = (lax.axis_index(a) for a in ("lat", "lon", "lev"))
    n_lon, n_lev = lax.axis_size("lon"), lax.axis_size("lev")
    assert n_lev == 8
    at_z, at_x = lax.div(lev, 2), lax.rem(lev, 2)
    up = (lat, lon, lax.rem(lev + 1, n_lev))
    down = (lat, lon, lax.rem(lev + n_lev - 1, n_lev))
    right = (lat, lax.rem(lon + 1, n_lon), lev)
    left = (lat, lax.rem(lon + n_lon - 1, n_lon), lev)
    core = (1 - lat, lon, lev)
    above = (lat, lon, lax.rem(lev + 2, n_lev))
    beneath = (lat, lon, lax.rem(lev + n_lev - 2, n_lev))
    partner = (lat, lon, lev + 1 - 2 * at_x)

    barrier = pltpu.get_barrier_semaphore()
    early = (down, left, core)
    for peer in early:
        pl.semaphore_signal(barrier, inc=1, device_id=peer, device_id_type=MESH)

    def in_turn(i):
        return lax.rem(i + (chunks - 1), chunks)

    def load_field(k):
        start, stop = ((nx - width, nx), (0, width), (width, nx - width))[k]
        return pltpu.make_async_copy(
            field_hbm.at[:, start:stop], F.at[0, 1 : ny + 1, start + 1 : stop + 1], ld.at[k]
        )

    def load_crowding():
        return pltpu.make_async_copy(crowd_hbm, C, ld.at[3])

    for k in range(3):
        load_field(k).start()
    load_crowding().start()

    def arrived(rows, sem):
        columns = rows // nz
        deep = max(k for k in range(1, ny + 1) if columns % k == 0 and columns // k <= nx)
        part = F.at[0, :deep, : columns // deep]
        return pltpu.make_async_copy(part, part, sem)

    chunk_rows = 2 * width * (ny + nz)
    step_rows = chunks * chunk_rows + 2 * ny * nz

    def remote(src, dst, send, recv, to):
        return pltpu.make_async_remote_copy(
            src_ref=src, dst_ref=dst, send_sem=send, recv_sem=recv, device_id=to, device_id_type=MESH
        )

    def faces(p, c):
        inside = pl.ds(c * width + 1, width)
        sems = (f_send.at[p], f_recv.at[p, c])
        return (
            remote(S.at[p, 1, c], H.at[p, 0, c], *sems, up),
            remote(S.at[p, 0, c], H.at[p, 1, c], *sems, down),
            remote(F.at[p, ny, inside], F.at[p, 0, inside], *sems, core),
            remote(F.at[p, 1, inside], F.at[p, ny + 1, inside], *sems, core),
        )

    def right_face(p):
        rows = pl.ds(1, ny)
        return remote(F.at[p, rows, nx], F.at[p, rows, 0], f_send.at[p], x_recv.at[p, 0], right)

    def left_face(p):
        rows = pl.ds(1, ny)
        return remote(F.at[p, rows, 1], F.at[p, rows, nx + 1], f_send.at[p], x_recv.at[p, 1], left)

    def start_faces(p, c, onward=True, back=True):
        if onward:

            @pl.when(c == chunks - 1)
            def _():
                right_face(p).start()

        if back:

            @pl.when(c == 0)
            def _():
                left_face(p).start()

        ahead_up, ahead_down, upper, lower = faces(p, c)
        for copy in onward * (ahead_up, upper, lower) + back * (ahead_down,):
            copy.start()

    def await_faces(p, c):
        arrived(chunk_rows, f_recv.at[p, c]).wait()

        @pl.when(c == 0)
        def _():
            right_face(p).wait_recv()

        @pl.when(c == chunks - 1)
        def _():
            left_face(p).wait_recv()

    def await_sent(p):
        arrived(step_rows, f_send.at[p]).wait()

    groups = width // GROUP

    def over_groups(c, body):
        def row(y, carry):
            def group(g, inner):
                body(y, g * GROUP, c * width + g * GROUP)
                return inner

            return lax.fori_loop(0, groups, group, carry)

        lax.fori_loop(0, ny, row, 0)

    def compute(step, c):
        p = step % 2
        level = lax.broadcasted_iota(jnp.int32, (nz, 128), 0)

        def body(y, g, x):
            columns = [F[p, y + 1, x + j] for j in range(GROUP + 2)]
            for j in range(GROUP):
                middle = columns[j + 1]
                low = H[p, 0, c, y, pl.ds(g + j, 1), :]
                high = H[p, 1, c, y, pl.ds(g + j, 1), :]
                under = jnp.where(level == 0, low, pltpu.roll(middle, 1, 0))
                over = jnp.where(level == nz - 1, high, pltpu.roll(middle, nz - 1, 0))
                total = columns[j] + columns[j + 2] + F[p, y, x + j + 1] + F[p, y + 2, x + j + 1] + under + over
                new = 0.1 * total + middle * (0.6 - 0.2 * (middle * C[y, x + j]))
                if step < STEPS - 1:
                    F[1 - p, y + 1, x + j + 1] = new
                    S[1 - p, 0, c, y, pl.ds(g + j, 1), :] = new[0:1]
                    S[1 - p, 1, c, y, pl.ds(g + j, 1), :] = new[nz - 1 : nz]
                else:
                    end[y, x + j] = new
                    here = new
                    reach = 1
                    while reach < nz:
                        here = here + jnp.where(level >= reach, pltpu.roll(here, reach, 0), 0.0)
                        reach *= 2
                    pot[y, x + j] = here * scale
                    T[c, y, pl.ds(g + j, 1), :] = here[nz - 1 : nz]

        over_groups(c, body)

    def prepare(c):
        def body(y, g, x):
            for j in range(GROUP):
                value = F[0, y + 1, x + j + 1]
                S[0, 0, c, y, pl.ds(g + j, 1), :] = value[0:1]
                S[0, 1, c, y, pl.ds(g + j, 1), :] = value[nz - 1 : nz]

        over_groups(c, body)

    load_field(0).wait()
    prepare(chunks - 1)
    pl.semaphore_wait(barrier, len(early))
    pl.semaphore_signal(met.at[0], inc=1, device_id=up, device_id_type=MESH)
    pl.semaphore_signal(met.at[1], inc=1, device_id=right, device_id_type=MESH)
    start_faces(0, chunks - 1, back=False)
    load_field(1).wait()
    prepare(0)
    start_faces(0, 0, back=False)
    load_field(2).wait()

    def first_onward(c, carry):
        prepare(c)
        start_faces(0, c, back=False)
        return carry

    def first_back(c, carry):
        start_faces(0, c, onward=False)
        return carry

    def first_both(c, carry):
        prepare(c)
        start_faces(0, c)
        return carry

    lax.fori_loop(1, ahead, first_onward, 0)
    pl.semaphore_wait(met.at[0], 1)
    pl.semaphore_wait(met.at[1], 1)
    start_faces(0, chunks - 1, onward=False)
    lax.fori_loop(0, ahead, first_back, 0)
    lax.fori_loop(ahead, chunks - 1, first_both, 0)

    def sent_on(src, dst, k, c, to):
        return remote(src.at[c], dst.at[c], q_send.at[k], q_recv.at[k, c], to)

    def across(c):
        return remote(X.at[c], B.at[c], b_send, b_recv.at[c], partner)

    def chain_own(c):
        @pl.when(at_z < 2)
        def _():
            sent_on(T, Q, 0, c, above).start()

        @pl.when(at_z == 0)
        def _():
            sent_on(T, Q, 1, c, beneath).start()

    def chain_first(c):
        @pl.when(at_z == 1)
        def _():
            sent_on(T, Q, 0, c, above).wait_recv()

        @pl.when(at_z == 2)
        def _():
            sent_on(T, Q, 0, c, above).wait_recv()
            U[c] = Q[c] + T[c]
            sent_on(U, R, 0, c, above).start()

        @pl.when(at_z == 3)
        def _():
            sent_on(T, Q, 1, c, beneath).wait_recv()
            sent_on(Q, R, 1, c, beneath).start()

    def chain_second(c):
        @pl.when(at_z == 0)
        def _():
            V[c] = jnp.zeros(V.shape[1:], V.dtype)

        @pl.when(at_z == 1)
        def _():
            V[c] = Q[c]

        @pl.when(at_z == 2)
        def _():
            sent_on(Q, R, 1, c, beneath).wait_recv()
            V[c] = Q[c] + R[c]

        @pl.when(at_z == 3)
        def _():
            sent_on(U, R, 0, c, above).wait_recv()
            V[c] = Q[c] + R[c]

        before = V[c]
        X[c] = jnp.where(at_x == 0, before + T[c], before)
        across(c).start()

    for step in range(STEPS):
        p = step % 2
        if step == 0:
            load_crowding().wait()
        else:
            await_sent(1 - p)

        def advance(i, carry):
            c = in_turn(i)
            await_faces(p, c)
            compute(step, c)
            if step < STEPS - 1:
                start_faces(1 - p, c)
            else:
                chain_own(c)

                @pl.when(i >= lag)
                def _():
                    chain_first(in_turn(i - lag))

                @pl.when(i >= 2 * lag)
                def _():
                    chain_second(in_turn(i - 2 * lag))

            return carry

        lax.fori_loop(0, chunks, advance, 0)

    def last_first(i, carry):
        chain_first(in_turn(i))
        return carry

    def last_second(i, carry):
        chain_second(in_turn(i))
        return carry

    lax.fori_loop(chunks - lag, chunks, last_first, 0)
    lax.fori_loop(chunks - 2 * lag, chunks, last_second, 0)

    def finish(i, carry):
        c = in_turn(i)
        across(c).wait_recv()
        V[c] = (V[c] + B[c]) * scale

        def body(y, g, x):
            for j in range(GROUP):
                pot[y, x + j] = pot[y, x + j] + V[c, y, pl.ds(g + j, 1), :]

        over_groups(c, body)
        return carry

    lax.fori_loop(0, chunks, finish, 0)

    await_sent((STEPS - 1) % 2)
    pltpu.make_async_copy(X, X, b_send).wait()

    @pl.when(at_z != 3)
    def _():
        pltpu.make_async_copy(T, T, q_send.at[0]).wait()

    @pl.when((at_z == 0) | (at_z == 3))
    def _():
        pltpu.make_async_copy(T, T, q_send.at[1]).wait()


def put_out(pot, end, pot_out, end_out, sems):
    pieces = sems.shape[1]
    depth = pot.shape[0] // pieces
    copies = [
        pltpu.make_async_copy(src.at[pl.ds(k * depth, depth)], dst.at[pl.ds(k * depth, depth)], sems.at[i, k])
        for k in range(pieces)
        for i, (src, dst) in enumerate(((pot, pot_out), (end, end_out)))
    ]
    for copy in copies:
        copy.start()
    for copy in copies:
        copy.wait()


def per_device(field_values, crowding):
    ny, nx, nz, lanes = field_values.shape
    width = 8
    chunks = nx // width
    scale = 1.0 / (nz * lax.axis_size("lev"))
    f32 = jnp.float32
    plane = (chunks, ny, width, lanes)
    dma = pltpu.SemaphoreType.DMA
    hbm = pl.BlockSpec(memory_space=pltpu.HBM)
    vmem = pl.BlockSpec(memory_space=pltpu.VMEM)
    results = pl.pallas_call(
        functools.partial(kernel, width, scale),
        out_shape=(pltpu.VMEM(field_values.shape, f32), pltpu.VMEM(field_values.shape, f32)),
        in_specs=[hbm, hbm],
        out_specs=(vmem, vmem),
        scratch_shapes=[
            pltpu.VMEM((2, ny + 2, nx + 2, nz, lanes), f32),
            pltpu.VMEM(field_values.shape, f32),
            pltpu.VMEM((2, 2) + plane, f32),
            pltpu.VMEM((2, 2) + plane, f32),
            pltpu.VMEM(plane, f32),
            pltpu.VMEM(plane, f32),
            pltpu.VMEM(plane, f32),
            pltpu.VMEM(plane, f32),
            pltpu.VMEM(plane, f32),
            pltpu.VMEM(plane, f32),
            pltpu.VMEM(plane, f32),
            pltpu.SemaphoreType.REGULAR((2,)),
            dma((4,)),
            dma((2,)), dma((2, chunks)), dma((2, 2)),
            dma((2,)), dma((2, chunks)),
            dma, dma((chunks,)),
        ],
        compiler_params=pltpu.CompilerParams(
            collective_id=0, has_side_effects=True, vmem_limit_bytes=42 * 2**20
        ),
    )(field_values, crowding)
    shape = jax.ShapeDtypeStruct(field_values.shape, f32)
    pieces = 4
    return tuple(pl.pallas_call(
        put_out,
        out_shape=(shape, shape),
        in_specs=[vmem, vmem],
        out_specs=(hbm, hbm),
        scratch_shapes=[dma((2, pieces))],
        compiler_params=pltpu.CompilerParams(vmem_limit_bytes=2**20),
    )(*results))


def solution(mesh):
    spec = P("lat", "lon", "lev", None)
    return jax.shard_map(
        per_device, mesh=mesh, in_specs=(spec, spec), out_specs=(spec, spec), check_vma=False
    )
```

```python
import functools

import jax
import jax.numpy as jnp
from jax import lax
from jax.experimental import pallas as pl
from jax.experimental.pallas import tpu as pltpu
from jax.sharding import PartitionSpec as P

STEPS = 4
GROUP = 8
FIRST = 2
SECOND = 5
LATE = 5
DIRECT = 3
MESH = pl.DeviceIdType.MESH


def kernel(
    width, scale, field_hbm, crowd_hbm, pot, end, VL, XL,
    F, C, H, S, T, Q, R, U, V, X, B,
    met, ld, f_send, f_recv, x_recv, q_send, q_recv, b_send,
):
    ny, nx, nz, _ = field_hbm.shape
    chunks = nx // width
    ahead = chunks // 2
    late_from = chunks - 1 - LATE
    direct_from = chunks - 1 - DIRECT
    lat, lon, lev = (lax.axis_index(a) for a in ("lat", "lon", "lev"))
    n_lon, n_lev = lax.axis_size("lon"), lax.axis_size("lev")
    assert n_lev == 8
    at_z, at_x = lax.div(lev, 2), lax.rem(lev, 2)
    up = (lat, lon, lax.rem(lev + 1, n_lev))
    down = (lat, lon, lax.rem(lev + n_lev - 1, n_lev))
    right = (lat, lax.rem(lon + 1, n_lon), lev)
    left = (lat, lax.rem(lon + n_lon - 1, n_lon), lev)
    core = (1 - lat, lon, lev)
    opposite = (lat, lon, lax.rem(lev + n_lev // 2, n_lev))
    above = (lat, lon, lax.rem(lev + 2, n_lev))
    beneath = (lat, lon, lax.rem(lev + n_lev - 2, n_lev))
    partner = (lat, lon, lev + 1 - 2 * at_x)

    barrier = pltpu.get_barrier_semaphore()
    odd = lax.rem(lon, 2)

    def signal(sem, to):
        pl.semaphore_signal(sem, inc=1, device_id=to, device_id_type=MESH)

    signal(barrier, down)
    signal(barrier, core)

    @pl.when(odd == 0)
    def _():
        signal(barrier, right)
        signal(barrier, left)


    def in_turn(i):
        return lax.rem(i + (chunks - 1), chunks)

    def load_field(k):
        start, stop = ((nx - width, nx), (0, width), (width, nx - width))[k]
        return pltpu.make_async_copy(
            field_hbm.at[:, start:stop], F.at[0, 1 : ny + 1, start + 1 : stop + 1], ld.at[k]
        )

    def load_crowding():
        return pltpu.make_async_copy(crowd_hbm, C, ld.at[3])

    for k in range(3):
        load_field(k).start()

    def arrived(rows, sem):
        columns = rows // nz
        deep = max(k for k in range(1, ny + 1) if columns % k == 0 and columns // k <= nx)
        part = F.at[0, :deep, : columns // deep]
        return pltpu.make_async_copy(part, part, sem)

    chunk_rows = 2 * width * (ny + nz)
    step_rows = chunks * chunk_rows + 2 * ny * nz

    def remote(src, dst, send, recv, to):
        return pltpu.make_async_remote_copy(
            src_ref=src, dst_ref=dst, send_sem=send, recv_sem=recv, device_id=to, device_id_type=MESH
        )

    def faces(p, c):
        inside = pl.ds(c * width + 1, width)
        sems = (f_send.at[p], f_recv.at[p, c])
        return (
            remote(S.at[p, 1, c], H.at[p, 0, c], *sems, up),
            remote(S.at[p, 0, c], H.at[p, 1, c], *sems, down),
            remote(F.at[p, ny, inside], F.at[p, 0, inside], *sems, core),
            remote(F.at[p, 1, inside], F.at[p, ny + 1, inside], *sems, core),
        )

    def right_face(p):
        rows = pl.ds(1, ny)
        return remote(F.at[p, rows, nx], F.at[p, rows, 0], f_send.at[p], x_recv.at[p, 0], right)

    def left_face(p):
        rows = pl.ds(1, ny)
        return remote(F.at[p, rows, 1], F.at[p, rows, nx + 1], f_send.at[p], x_recv.at[p, 1], left)

    def start_faces(p, c, onward=True, back=True, columns=True):
        if columns:

            @pl.when(c == chunks - 1)
            def _():
                right_face(p).start()

            @pl.when(c == 0)
            def _():
                left_face(p).start()

        ahead_up, ahead_down, upper, lower = faces(p, c)
        for copy in onward * (ahead_up, upper, lower) + back * (ahead_down,):
            copy.start()

    def await_faces(p, c):
        arrived(chunk_rows, f_recv.at[p, c]).wait()

        @pl.when(c == 0)
        def _():
            right_face(p).wait_recv()

        @pl.when(c == chunks - 1)
        def _():
            left_face(p).wait_recv()

    def await_sent(p):
        arrived(step_rows, f_send.at[p]).wait()

    groups = width // GROUP

    def over_groups(c, body):
        def row(y, carry):
            def group(g, inner):
                body(y, g * GROUP, c * width + g * GROUP)
                return inner

            return lax.fori_loop(0, groups, group, carry)

        lax.fori_loop(0, ny, row, 0)

    def compute(step, c):
        p = step % 2
        level = lax.broadcasted_iota(jnp.int32, (nz, 128), 0)

        def body(y, g, x):
            columns = [F[p, y + 1, x + j] for j in range(GROUP + 2)]
            for j in range(GROUP):
                middle = columns[j + 1]
                low = H[p, 0, c, y, pl.ds(g + j, 1), :]
                high = H[p, 1, c, y, pl.ds(g + j, 1), :]
                under = jnp.where(level == 0, low, pltpu.roll(middle, 1, 0))
                over = jnp.where(level == nz - 1, high, pltpu.roll(middle, nz - 1, 0))
                total = columns[j] + columns[j + 2] + F[p, y, x + j + 1] + F[p, y + 2, x + j + 1] + under + over
                new = 0.1 * total + middle * (0.6 - 0.2 * (middle * C[y, x + j]))
                if step < STEPS - 1:
                    F[1 - p, y + 1, x + j + 1] = new
                    S[1 - p, 0, c, y, pl.ds(g + j, 1), :] = new[0:1]
                    S[1 - p, 1, c, y, pl.ds(g + j, 1), :] = new[nz - 1 : nz]
                else:
                    end[y, x + j] = new
                    here = new
                    reach = 1
                    while reach < nz:
                        here = here + jnp.where(level >= reach, pltpu.roll(here, reach, 0), 0.0)
                        reach *= 2
                    pot[y, x + j] = here * scale
                    T[c, y, pl.ds(g + j, 1), :] = here[nz - 1 : nz]

        over_groups(c, body)

    def prepare(c):
        def body(y, g, x):
            for j in range(GROUP):
                value = F[0, y + 1, x + j + 1]
                S[0, 0, c, y, pl.ds(g + j, 1), :] = value[0:1]
                S[0, 1, c, y, pl.ds(g + j, 1), :] = value[nz - 1 : nz]

        over_groups(c, body)

    load_field(0).wait()
    prepare(chunks - 1)
    pl.semaphore_wait(barrier, 2 + 2 * odd)
    signal(met.at[0], up)

    @pl.when(odd == 1)
    def _():
        signal(met.at[1], left)
        signal(met.at[2], right)

    start_faces(0, chunks - 1, back=False, columns=False)
    load_field(1).wait()
    prepare(0)
    start_faces(0, 0, back=False, columns=False)
    load_field(2).wait()

    def first_onward(c, carry):
        prepare(c)
        start_faces(0, c, back=False, columns=False)
        return carry

    def first_back(c, carry):
        start_faces(0, c, onward=False, columns=False)
        return carry

    def first_both(c, carry):
        prepare(c)
        start_faces(0, c, columns=False)
        return carry

    lax.fori_loop(1, ahead, first_onward, 0)

    @pl.when(odd == 0)
    def _():
        pl.semaphore_wait(met.at[1], 1)
        pl.semaphore_wait(met.at[2], 1)

    right_face(0).start()
    left_face(0).start()
    pl.semaphore_wait(met.at[0], 1)
    start_faces(0, chunks - 1, onward=False, columns=False)
    lax.fori_loop(0, ahead, first_back, 0)
    lax.fori_loop(ahead, chunks - 1, first_both, 0)
    load_crowding().start()

    def sent_on(src, dst, k, c, to):
        return remote(src.at[c], dst.at[c], q_send.at[k], q_recv.at[k, c], to)

    def across(c):
        return remote(X.at[c], B.at[c], b_send, f_recv.at[0, c], partner)

    def pass_across(c, before):
        onward = jnp.where(at_x == 0, before + T[c], before)

        @pl.when((c < late_from) | (c == chunks - 1))
        def _():
            V[c] = before
            X[c] = onward
            across(c).start()

        @pl.when((c >= late_from) & (c < chunks - 1))
        def _():
            VL[c - late_from] = before
            XL[c - late_from] = onward

    def goes_direct(c):
        return (c >= direct_from) & (c < chunks - 1)

    def direct(c):
        return remote(T.at[c], R.at[c], q_send.at[1], q_recv.at[1, c], opposite)

    def chain_own(c):
        @pl.when(at_z < 2)
        def _():
            sent_on(T, Q, 0, c, above).start()

        @pl.when(at_z == 0)
        def _():

            @pl.when(goes_direct(c))
            def _():
                direct(c).start()

            sent_on(T, Q, 1, c, beneath).start()
            pass_across(c, jnp.zeros(V.shape[1:], V.dtype))

    def chain_first(c):
        @pl.when(at_z == 1)
        def _():
            sent_on(T, Q, 0, c, above).wait_recv()
            pass_across(c, Q[c])

        @pl.when(at_z == 2)
        def _():
            sent_on(T, Q, 0, c, above).wait_recv()
            U[c] = Q[c] + T[c]
            sent_on(U, R, 0, c, above).start()

        @pl.when(at_z == 3)
        def _():
            sent_on(T, Q, 1, c, beneath).wait_recv()

            @pl.when(jnp.logical_not(goes_direct(c)))
            def _():
                sent_on(Q, R, 1, c, beneath).start()


    def chain_second(c):
        @pl.when(at_z == 2)
        def _():
            sent_on(Q, R, 1, c, beneath).wait_recv()
            pass_across(c, Q[c] + R[c])

        @pl.when(at_z == 3)
        def _():
            sent_on(U, R, 0, c, above).wait_recv()
            pass_across(c, Q[c] + R[c])

    for step in range(STEPS):
        p = step % 2
        if step == 0:
            load_crowding().wait()
        else:
            await_sent(1 - p)

        def advance(i, carry):
            c = in_turn(i)
            await_faces(p, c)
            compute(step, c)
            if step < STEPS - 1:
                start_faces(1 - p, c)
            else:
                chain_own(c)

                @pl.when(i >= FIRST)
                def _():
                    chain_first(in_turn(i - FIRST))

                @pl.when(i >= SECOND)
                def _():
                    chain_second(in_turn(i - SECOND))

            return carry

        lax.fori_loop(0, chunks, advance, 0)

    def last_first(i, carry):
        chain_first(in_turn(i))
        return carry

    def last_second(i, carry):
        chain_second(in_turn(i))
        return carry

    lax.fori_loop(chunks - FIRST, chunks, last_first, 0)
    lax.fori_loop(chunks - SECOND, chunks, last_second, 0)

    def finish(i, carry):
        c = in_turn(i)
        across(c).wait_recv()
        V[c] = (V[c] + B[c]) * scale

        def body(y, g, x):
            for j in range(GROUP):
                pot[y, x + j] = pot[y, x + j] + V[c, y, pl.ds(g + j, 1), :]

        over_groups(c, body)
        return carry

    lax.fori_loop(0, chunks - LATE, finish, 0)

    await_sent((STEPS - 1) % 2)
    sent = X.at[: chunks - LATE]
    pltpu.make_async_copy(sent, sent, b_send).wait()

    @pl.when(at_z != 3)
    def _():
        pltpu.make_async_copy(T, T, q_send.at[0]).wait()

    @pl.when(at_z == 0)
    def _():
        arrived((chunks + DIRECT) * ny * width, q_send.at[1]).wait()

    @pl.when(at_z == 3)
    def _():
        arrived((chunks - DIRECT) * ny * width, q_send.at[1]).wait()


def put_first(first, stop, pot, end, pot_out, end_out, sems):
    half = pot.shape[0] // 2
    nx = pot.shape[1]
    copies = []
    for k in range(2):
        rows = pl.ds(k * half, half)
        for src, dst, at in (
            (end, end_out, slice(None)),
            (pot, pot_out, slice(0, first)),
            (pot, pot_out, slice(stop, nx)),
        ):
            copies.append(pltpu.make_async_copy(src.at[rows, at], dst.at[rows, at], sems.at[len(copies)]))
    for copy in copies:
        copy.start()
    for copy in copies:
        copy.wait()


def put_late(first, width, scale, pot, VL, BL, pot_in, pot_out, held, sems):
    del pot_in
    ny = pot.shape[0]
    copies = []
    for k in range(LATE):
        def row(y, carry, k=k):
            below = (VL[k, y] + BL[k, y]) * scale
            for j in range(width):
                held[k, y, j] = pot[y, first + k * width + j] + below[j : j + 1]
            return carry

        lax.fori_loop(0, ny, row, 0)
        copies.append(
            pltpu.make_async_copy(held.at[k], pot_out.at[:, first + k * width : first + (k + 1) * width], sems.at[k])
        )
        copies[-1].start()
    for copy in copies:
        copy.wait()


def per_device(field_values, crowding):
    ny, nx, nz, lanes = field_values.shape
    width = 8
    chunks = nx // width
    scale = 1.0 / (nz * lax.axis_size("lev"))
    f32 = jnp.float32
    plane = (chunks, ny, width, lanes)
    dma = pltpu.SemaphoreType.DMA
    hbm = pl.BlockSpec(memory_space=pltpu.HBM)
    vmem = pl.BlockSpec(memory_space=pltpu.VMEM)
    results = pl.pallas_call(
        functools.partial(kernel, width, scale),
        out_shape=(pltpu.VMEM(field_values.shape, f32),) * 2 + (pltpu.VMEM((LATE,) + plane[1:], f32),) * 2,
        in_specs=[hbm, hbm],
        out_specs=(vmem,) * 4,
        scratch_shapes=[
            pltpu.VMEM((2, ny + 2, nx + 2, nz, lanes), f32),
            pltpu.VMEM(field_values.shape, f32),
            pltpu.VMEM((2, 2) + plane, f32),
            pltpu.VMEM((2, 2) + plane, f32),
            pltpu.VMEM(plane, f32),
            pltpu.VMEM(plane, f32),
            pltpu.VMEM(plane, f32),
            pltpu.VMEM(plane, f32),
            pltpu.VMEM(plane, f32),
            pltpu.VMEM(plane, f32),
            pltpu.VMEM(plane, f32),
            pltpu.SemaphoreType.REGULAR((3,)),
            dma((4,)),
            dma((2,)), dma((2, chunks)), dma((2, 2)),
            dma((2,)), dma((2, chunks)),
            dma,
        ],
        compiler_params=pltpu.CompilerParams(
            collective_id=0, has_side_effects=True, vmem_limit_bytes=42 * 2**20
        ),
    )(field_values, crowding)
    pot, end, before, onward = results
    shape = jax.ShapeDtypeStruct(field_values.shape, f32)
    n_lev = lax.axis_size("lev")
    first, stop = nx - width * (LATE + 1), nx - width
    across = lax.ppermute(onward, "lev", [(k, k ^ 1) for k in range(n_lev)])
    size = 4 * field_values.size
    pot_out, end_out = pl.pallas_call(
        functools.partial(put_first, first, stop),
        out_shape=(shape, shape),
        in_specs=[vmem, vmem],
        out_specs=(hbm, hbm),
        scratch_shapes=[dma((6,))],
        cost_estimate=pl.CostEstimate(flops=0, bytes_accessed=2 * size, transcendentals=0),
        compiler_params=pltpu.CompilerParams(vmem_limit_bytes=2**20),
    )(pot, end)
    pot_out = pl.pallas_call(
        functools.partial(put_late, first, width, scale),
        out_shape=shape,
        in_specs=[vmem, vmem, vmem, hbm],
        out_specs=hbm,
        scratch_shapes=[pltpu.VMEM((LATE, ny, width, nz, lanes), f32), dma((LATE,))],
        input_output_aliases={3: 0},
        compiler_params=pltpu.CompilerParams(vmem_limit_bytes=4 * 2**20),
    )(pot, before, across, pot_out)
    return pot_out, end_out


def solution(mesh):
    spec = P("lat", "lon", "lev", None)
    return jax.shard_map(
        per_device, mesh=mesh, in_specs=(spec, spec), out_specs=(spec, spec), check_vma=False
    )
```

```python
import functools

import jax
import jax.numpy as jnp
from jax import lax
from jax.experimental import pallas as pl
from jax.experimental.pallas import tpu as pltpu
from jax.sharding import PartitionSpec as P

STEPS = 4
GROUP = 8
FIRST = 2
SECOND = 5
LATE = 6
DIRECT = 2
MESH = pl.DeviceIdType.MESH


def kernel(
    width, scale, field_hbm, crowd_hbm, pot, end, VL, XL,
    F, C, H, S, T, Q, R, U, V, X, B,
    met, ld, f_send, f_recv, x_recv, q_send, q_recv, b_send,
):
    ny, nx, nz, _ = field_hbm.shape
    chunks = nx // width
    ahead = chunks // 2
    late_from = chunks - 1 - LATE
    direct_from = chunks - 1 - DIRECT
    lat, lon, lev = (lax.axis_index(a) for a in ("lat", "lon", "lev"))
    n_lon, n_lev = lax.axis_size("lon"), lax.axis_size("lev")
    assert n_lev == 8
    at_z, at_x = lax.div(lev, 2), lax.rem(lev, 2)
    up = (lat, lon, lax.rem(lev + 1, n_lev))
    down = (lat, lon, lax.rem(lev + n_lev - 1, n_lev))
    right = (lat, lax.rem(lon + 1, n_lon), lev)
    left = (lat, lax.rem(lon + n_lon - 1, n_lon), lev)
    core = (1 - lat, lon, lev)
    opposite = (lat, lon, lax.rem(lev + n_lev // 2, n_lev))
    above = (lat, lon, lax.rem(lev + 2, n_lev))
    beneath = (lat, lon, lax.rem(lev + n_lev - 2, n_lev))
    partner = (lat, lon, lev + 1 - 2 * at_x)

    barrier = pltpu.get_barrier_semaphore()
    odd = lax.rem(lon, 2)

    def signal(sem, to):
        pl.semaphore_signal(sem, inc=1, device_id=to, device_id_type=MESH)

    signal(barrier, down)
    signal(barrier, core)

    @pl.when(odd == 0)
    def _():
        signal(barrier, right)
        signal(barrier, left)


    def in_turn(i):
        return lax.rem(i + (chunks - 1), chunks)

    def load_field(k):
        start, stop = ((nx - width, nx), (0, width), (width, nx - width))[k]
        return pltpu.make_async_copy(
            field_hbm.at[:, start:stop], F.at[0, 1 : ny + 1, start + 1 : stop + 1], ld.at[k]
        )

    def load_crowding():
        return pltpu.make_async_copy(crowd_hbm, C, ld.at[3])

    for k in range(3):
        load_field(k).start()

    def arrived(rows, sem):
        columns = rows // nz
        deep = max(k for k in range(1, ny + 1) if columns % k == 0 and columns // k <= nx)
        part = F.at[0, :deep, : columns // deep]
        return pltpu.make_async_copy(part, part, sem)

    chunk_rows = 2 * width * (ny + nz)
    step_rows = chunks * chunk_rows + 2 * ny * nz

    def remote(src, dst, send, recv, to):
        return pltpu.make_async_remote_copy(
            src_ref=src, dst_ref=dst, send_sem=send, recv_sem=recv, device_id=to, device_id_type=MESH
        )

    def faces(p, c):
        inside = pl.ds(c * width + 1, width)
        sems = (f_send.at[p], f_recv.at[p, c])
        return (
            remote(S.at[p, 1, c], H.at[p, 0, c], *sems, up),
            remote(S.at[p, 0, c], H.at[p, 1, c], *sems, down),
            remote(F.at[p, ny, inside], F.at[p, 0, inside], *sems, core),
            remote(F.at[p, 1, inside], F.at[p, ny + 1, inside], *sems, core),
        )

    def right_face(p):
        rows = pl.ds(1, ny)
        return remote(F.at[p, rows, nx], F.at[p, rows, 0], f_send.at[p], x_recv.at[p, 0], right)

    def left_face(p):
        rows = pl.ds(1, ny)
        return remote(F.at[p, rows, 1], F.at[p, rows, nx + 1], f_send.at[p], x_recv.at[p, 1], left)

    def start_faces(p, c, onward=True, back=True, columns=True):
        if columns:

            @pl.when(c == chunks - 1)
            def _():
                right_face(p).start()

            @pl.when(c == 0)
            def _():
                left_face(p).start()

        ahead_up, ahead_down, upper, lower = faces(p, c)
        for copy in onward * (ahead_up, upper, lower) + back * (ahead_down,):
            copy.start()

    def await_faces(p, c):
        arrived(chunk_rows, f_recv.at[p, c]).wait()

        @pl.when(c == 0)
        def _():
            right_face(p).wait_recv()

        @pl.when(c == chunks - 1)
        def _():
            left_face(p).wait_recv()

    def await_sent(p):
        arrived(step_rows, f_send.at[p]).wait()

    groups = width // GROUP

    def over_groups(c, body):
        def row(y, carry):
            def group(g, inner):
                body(y, g * GROUP, c * width + g * GROUP)
                return inner

            return lax.fori_loop(0, groups, group, carry)

        lax.fori_loop(0, ny, row, 0)

    def compute(step, c):
        p = step % 2
        level = lax.broadcasted_iota(jnp.int32, (nz, 128), 0)

        def body(y, g, x):
            columns = [F[p, y + 1, x + j] for j in range(GROUP + 2)]
            for j in range(GROUP):
                middle = columns[j + 1]
                low = H[p, 0, c, y, pl.ds(g + j, 1), :]
                high = H[p, 1, c, y, pl.ds(g + j, 1), :]
                under = jnp.where(level == 0, low, pltpu.roll(middle, 1, 0))
                over = jnp.where(level == nz - 1, high, pltpu.roll(middle, nz - 1, 0))
                total = columns[j] + columns[j + 2] + F[p, y, x + j + 1] + F[p, y + 2, x + j + 1] + under + over
                new = 0.1 * total + middle * (0.6 - 0.2 * (middle * C[y, x + j]))
                if step < STEPS - 1:
                    F[1 - p, y + 1, x + j + 1] = new
                    S[1 - p, 0, c, y, pl.ds(g + j, 1), :] = new[0:1]
                    S[1 - p, 1, c, y, pl.ds(g + j, 1), :] = new[nz - 1 : nz]
                else:
                    end[y, x + j] = new
                    here = new
                    reach = 1
                    while reach < nz:
                        here = here + jnp.where(level >= reach, pltpu.roll(here, reach, 0), 0.0)
                        reach *= 2
                    pot[y, x + j] = here * scale
                    T[c, y, pl.ds(g + j, 1), :] = here[nz - 1 : nz]

        over_groups(c, body)

    def prepare(c):
        def body(y, g, x):
            for j in range(GROUP):
                value = F[0, y + 1, x + j + 1]
                S[0, 0, c, y, pl.ds(g + j, 1), :] = value[0:1]
                S[0, 1, c, y, pl.ds(g + j, 1), :] = value[nz - 1 : nz]

        over_groups(c, body)

    load_field(0).wait()
    prepare(chunks - 1)
    pl.semaphore_wait(barrier, 2 + 2 * odd)
    signal(met.at[0], up)

    @pl.when(odd == 1)
    def _():
        signal(met.at[1], left)
        signal(met.at[2], right)

    start_faces(0, chunks - 1, back=False, columns=False)
    load_field(1).wait()
    prepare(0)
    start_faces(0, 0, back=False, columns=False)
    load_field(2).wait()

    def first_onward(c, carry):
        prepare(c)
        start_faces(0, c, back=False, columns=False)
        return carry

    def first_back(c, carry):
        start_faces(0, c, onward=False, columns=False)
        return carry

    def first_both(c, carry):
        prepare(c)
        start_faces(0, c, columns=False)
        return carry

    lax.fori_loop(1, ahead, first_onward, 0)

    @pl.when(odd == 0)
    def _():
        pl.semaphore_wait(met.at[1], 1)
        pl.semaphore_wait(met.at[2], 1)

    right_face(0).start()
    left_face(0).start()
    pl.semaphore_wait(met.at[0], 1)
    start_faces(0, chunks - 1, onward=False, columns=False)
    lax.fori_loop(0, ahead, first_back, 0)
    lax.fori_loop(ahead, chunks - 1, first_both, 0)
    load_crowding().start()

    def sent_on(src, dst, k, c, to):
        return remote(src.at[c], dst.at[c], q_send.at[k], q_recv.at[k, c], to)

    def across(c):
        return remote(X.at[c], B.at[c], b_send, f_recv.at[0, c], partner)

    def pass_across(c, before):
        onward = jnp.where(at_x == 0, before + T[c], before)

        @pl.when((c < late_from) | (c == chunks - 1))
        def _():
            V[c] = before
            X[c] = onward
            across(c).start()

        @pl.when((c >= late_from) & (c < chunks - 1))
        def _():
            VL[c - late_from] = before
            XL[c - late_from] = onward

    def goes_direct(c):
        return (c >= direct_from) & (c < chunks - 1)

    def direct(c):
        return remote(T.at[c], R.at[c], q_send.at[1], q_recv.at[1, c], opposite)

    def chain_own(c):
        @pl.when(at_z < 2)
        def _():
            sent_on(T, Q, 0, c, above).start()

        @pl.when(at_z == 0)
        def _():

            @pl.when(goes_direct(c))
            def _():
                direct(c).start()

            sent_on(T, Q, 1, c, beneath).start()
            pass_across(c, jnp.zeros(V.shape[1:], V.dtype))

    def chain_first(c):
        @pl.when(at_z == 1)
        def _():
            sent_on(T, Q, 0, c, above).wait_recv()
            pass_across(c, Q[c])

        @pl.when(at_z == 2)
        def _():
            sent_on(T, Q, 0, c, above).wait_recv()
            U[c] = Q[c] + T[c]
            sent_on(U, R, 0, c, above).start()

        @pl.when(at_z == 3)
        def _():
            sent_on(T, Q, 1, c, beneath).wait_recv()

            @pl.when(jnp.logical_not(goes_direct(c)))
            def _():
                sent_on(Q, R, 1, c, beneath).start()


    def chain_second(c):
        @pl.when(at_z == 2)
        def _():
            sent_on(Q, R, 1, c, beneath).wait_recv()
            pass_across(c, Q[c] + R[c])

        @pl.when(at_z == 3)
        def _():
            sent_on(U, R, 0, c, above).wait_recv()
            pass_across(c, Q[c] + R[c])

    for step in range(STEPS):
        p = step % 2
        if step == 0:
            load_crowding().wait()
        else:
            await_sent(1 - p)

        def advance(i, carry):
            c = in_turn(i)
            await_faces(p, c)
            compute(step, c)
            if step < STEPS - 1:
                start_faces(1 - p, c)
            else:
                chain_own(c)

                @pl.when(i >= FIRST)
                def _():
                    chain_first(in_turn(i - FIRST))

                @pl.when(i >= SECOND)
                def _():
                    chain_second(in_turn(i - SECOND))

            return carry

        lax.fori_loop(0, chunks, advance, 0)

    def last_first(i, carry):
        chain_first(in_turn(i))
        return carry

    def last_second(i, carry):
        chain_second(in_turn(i))
        return carry

    lax.fori_loop(chunks - FIRST, chunks, last_first, 0)
    lax.fori_loop(chunks - SECOND, chunks, last_second, 0)

    def finish(i, carry):
        c = in_turn(i)
        across(c).wait_recv()
        V[c] = (V[c] + B[c]) * scale

        def body(y, g, x):
            for j in range(GROUP):
                pot[y, x + j] = pot[y, x + j] + V[c, y, pl.ds(g + j, 1), :]

        over_groups(c, body)
        return carry

    lax.fori_loop(0, chunks - LATE, finish, 0)

    await_sent((STEPS - 1) % 2)
    sent = X.at[: chunks - LATE]
    pltpu.make_async_copy(sent, sent, b_send).wait()

    @pl.when(at_z != 3)
    def _():
        pltpu.make_async_copy(T, T, q_send.at[0]).wait()

    @pl.when(at_z == 0)
    def _():
        arrived((chunks + DIRECT) * ny * width, q_send.at[1]).wait()

    @pl.when(at_z == 3)
    def _():
        arrived((chunks - DIRECT) * ny * width, q_send.at[1]).wait()


def put_first(first, stop, pot, end, pot_out, end_out, sems):
    half = pot.shape[0] // 2
    nx = pot.shape[1]
    copies = []
    for k in range(2):
        rows = pl.ds(k * half, half)
        for src, dst, at in (
            (end, end_out, slice(None)),
            (pot, pot_out, slice(0, first)),
            (pot, pot_out, slice(stop, nx)),
        ):
            copies.append(pltpu.make_async_copy(src.at[rows, at], dst.at[rows, at], sems.at[len(copies)]))
    for copy in copies:
        copy.start()
    for copy in copies:
        copy.wait()


def put_late(first, width, scale, pot, VL, BL, pot_in, pot_out, held, sems):
    del pot_in
    ny = pot.shape[0]
    copies = []
    for k in range(LATE):
        def rows(turn, carry, k=k):
            for part in range(4):
                y = turn * 4 + part
                below = (VL[k, y] + BL[k, y]) * scale
                for j in range(width):
                    held[k, y, j] = pot[y, first + k * width + j] + below[j : j + 1]
            return carry

        lax.fori_loop(0, ny // 4, rows, 0)
        copies.append(
            pltpu.make_async_copy(held.at[k], pot_out.at[:, first + k * width : first + (k + 1) * width], sems.at[k])
        )
        copies[-1].start()
    for copy in copies:
        copy.wait()


def per_device(field_values, crowding):
    ny, nx, nz, lanes = field_values.shape
    width = 8
    chunks = nx // width
    scale = 1.0 / (nz * lax.axis_size("lev"))
    f32 = jnp.float32
    plane = (chunks, ny, width, lanes)
    dma = pltpu.SemaphoreType.DMA
    hbm = pl.BlockSpec(memory_space=pltpu.HBM)
    vmem = pl.BlockSpec(memory_space=pltpu.VMEM)
    results = pl.pallas_call(
        functools.partial(kernel, width, scale),
        out_shape=(pltpu.VMEM(field_values.shape, f32),) * 2 + (pltpu.VMEM((LATE,) + plane[1:], f32),) * 2,
        in_specs=[hbm, hbm],
        out_specs=(vmem,) * 4,
        scratch_shapes=[
            pltpu.VMEM((2, ny + 2, nx + 2, nz, lanes), f32),
            pltpu.VMEM(field_values.shape, f32),
            pltpu.VMEM((2, 2) + plane, f32),
            pltpu.VMEM((2, 2) + plane, f32),
            pltpu.VMEM(plane, f32),
            pltpu.VMEM(plane, f32),
            pltpu.VMEM(plane, f32),
            pltpu.VMEM(plane, f32),
            pltpu.VMEM(plane, f32),
            pltpu.VMEM(plane, f32),
            pltpu.VMEM(plane, f32),
            pltpu.SemaphoreType.REGULAR((3,)),
            dma((4,)),
            dma((2,)), dma((2, chunks)), dma((2, 2)),
            dma((2,)), dma((2, chunks)),
            dma,
        ],
        compiler_params=pltpu.CompilerParams(
            collective_id=0, has_side_effects=True, vmem_limit_bytes=42 * 2**20
        ),
    )(field_values, crowding)
    pot, end, before, onward = results
    shape = jax.ShapeDtypeStruct(field_values.shape, f32)
    n_lev = lax.axis_size("lev")
    first, stop = nx - width * (LATE + 1), nx - width
    across = lax.ppermute(onward, "lev", [(k, k ^ 1) for k in range(n_lev)])
    size = 4 * field_values.size
    pot_out, end_out = pl.pallas_call(
        functools.partial(put_first, first, stop),
        out_shape=(shape, shape),
        in_specs=[vmem, vmem],
        out_specs=(hbm, hbm),
        scratch_shapes=[dma((6,))],
        cost_estimate=pl.CostEstimate(flops=0, bytes_accessed=2 * size, transcendentals=0),
        compiler_params=pltpu.CompilerParams(vmem_limit_bytes=2**20),
    )(pot, end)
    pot_out = pl.pallas_call(
        functools.partial(put_late, first, width, scale),
        out_shape=shape,
        in_specs=[vmem, vmem, vmem, hbm],
        out_specs=hbm,
        scratch_shapes=[pltpu.VMEM((LATE, ny, width, nz, lanes), f32), dma((LATE,))],
        input_output_aliases={3: 0},
        compiler_params=pltpu.CompilerParams(vmem_limit_bytes=4 * 2**20),
    )(pot, before, across, pot_out)
    return pot_out, end_out


def solution(mesh):
    spec = P("lat", "lon", "lev", None)
    return jax.shard_map(
        per_device, mesh=mesh, in_specs=(spec, spec), out_specs=(spec, spec), check_vma=False
    )
```
